256 devices in a mesh: dp: 32 (over y, x, core), mp: 8 (over z).
Axes of the slice: x: 4, y: 4, z: 8, core: 2. Of those that a mesh axis runs over, the one named last changes fastest.
Arguments:
- clean: bfloat16 [128, 256, 1536], P('dp', None, 'mp'), may hold values from -6 to 6
- noise: bfloat16 [128, 256, 1536], P('dp', None, 'mp'), may hold values from -6 to 6
- teacher_first: bfloat16 [128, 256, 1536], P('dp', None, 'mp'), may hold values from -6 to 6
- teacher_second: bfloat16 [128, 256, 1536], P('dp', None, 'mp'), may hold values from -6 to 6
- step_index: int32 [128], P('dp'), may hold values from 8 to 32
- teacher_count: int32 [128], P('dp'), may hold values from 64 to 256
- up_master: float32 [1536, 6144], P('dp', 'mp'), may hold values from -6 to 6
- down_master: float32 [1536, 6144], P('dp', 'mp'), may hold values from -6 to 6
- up_moment: float32 [1536, 6144], P('dp', 'mp'), may hold values from -1.8 to 1.8
- down_moment: float32 [1536, 6144], P('dp', 'mp'), may hold values from -1.8 to 1.8
- up_second: float32 [1536, 6144], P('dp', 'mp'), may hold values from 0.002 to 0.032
- down_second: float32 [1536, 6144], P('dp', 'mp'), may hold values from 0.002 to 0.032
Outputs:
- new_up_master: float32 [1536, 6144], P('dp', 'mp')
- new_down_master: float32 [1536, 6144], P('dp', 'mp')
- new_up_moment: float32 [1536, 6144], P('dp', 'mp')
- new_down_moment: float32 [1536, 6144], P('dp', 'mp')
- new_up_second: float32 [1536, 6144], P('dp', 'mp')
- new_down_second: float32 [1536, 6144], P('dp', 'mp')
- loss_mean: float32 [], replicated
The draws below stay inside these ranges and needn't reach their ends.
Inputs may be any that keep to these rules, and one draw needn't show every extreme that they name: `step_index`: student step k with 2k at most the sample's teacher_count.
All inputs are finite; a program needn't handle non-finite values.
Results may differ from the reference program's by a relative error of at most 0.002.
Values may be sent and summed in bfloat16 or wider, within the bound.
No kernel may reach another device: no remote copies, remote signals or barrier semaphores. Data moves between devices by JAX's collectives and lax.ppermute only.
A program may use at most 64 MiB of HBM per device.

```python
import math
import jax
import jax.numpy as jnp
from jax import lax

D = 1536
FF = 6144
TOK = 256
SAMPLES = 128
N_MP = 8


def with_ends(drawn, key, smallest, top_value):
    shape = drawn.shape
    spot = [jax.random.randint(jax.random.fold_in(key, axis), (), 0, shape[axis]) for axis in range(len(shape))]
    drawn = drawn.at[tuple(spot)].set(smallest)
    longest = shape.index(max(shape))
    spot[longest] = (spot[longest] + 1) % shape[longest]
    return drawn.at[tuple(spot)].set(top_value)


def steps_of(rng, extent, shards, low, largest):
    factor_of = 1.0
    for position, shards_of in shards:
        heights = jax.random.uniform(jax.random.fold_in(jax.random.fold_in(rng, 6), position), (shards_of,), jnp.float32, low / len(shards), largest / len(shards))
        factor_of = factor_of * jnp.repeat(jnp.exp(heights), extent[position] // shards_of).reshape((-1,) + (1,) * (len(extent) - 1 - position))
    return factor_of


def normal_values(own_key, extent, width, most, split=(), kind=jnp.bfloat16):
    level = steps_of(own_key, extent, split, -0.22, 0.18) if split else 1.0
    array = jax.random.normal(own_key, extent, jnp.float32) * width * level
    return jnp.minimum(jnp.maximum(array, -most), most).astype(kind)


def setup_inputs(seed: int = 0) -> dict:
    key_of = jax.random.split(jax.random.key(seed), 13)
    return {
        "clean": normal_values(key_of[0], (SAMPLES, TOK, D), 1.0, 6.0, ((0, 32), (2, 8))),
        "noise": normal_values(key_of[1], (SAMPLES, TOK, D), 1.0, 6.0, ((0, 32), (2, 8))),
        "teacher_first": normal_values(key_of[2], (SAMPLES, TOK, D), 1.0, 6.0, ((0, 32), (2, 8))),
        "teacher_second": normal_values(key_of[3], (SAMPLES, TOK, D), 1.0, 6.0, ((0, 32), (2, 8))),
        "step_index": with_ends(jax.random.randint(key_of[4], (SAMPLES,), 8, 33), jax.random.fold_in(key_of[4], 1), 8, 32).astype(jnp.int32),
        "teacher_count": with_ends(jax.random.randint(key_of[5], (SAMPLES,), 64, 257), jax.random.fold_in(key_of[5], 1), 64, 256).astype(jnp.int32),
        "up_master": normal_values(key_of[6], (D, FF), 1.0, 6.0, ((0, 32), (1, 8)), jnp.float32),
        "down_master": normal_values(key_of[7], (D, FF), 1.0, 6.0, ((0, 32), (1, 8)), jnp.float32),
        "up_moment": normal_values(key_of[8], (D, FF), 0.3, 1.8, ((0, 32), (1, 8)), jnp.float32),
        "down_moment": normal_values(key_of[9], (D, FF), 0.3, 1.8, ((0, 32), (1, 8)), jnp.float32),
        "up_second": jnp.clip(jnp.exp(math.log(0.032) - 2.7725887 * jax.random.uniform(key_of[10], (D, FF), jnp.float32) ** steps_of(key_of[10], (D, FF), ((0, 32), (1, 8)), -0.2, 0.2)), 0.002, 0.032),
        "down_second": jnp.clip(jnp.exp(math.log(0.032) - 2.7725887 * jax.random.uniform(key_of[11], (D, FF), jnp.float32) ** steps_of(key_of[11], (D, FF), ((0, 32), (1, 8)), -0.2, 0.2)), 0.002, 0.032),
    }


adam_count = 100.0
learn_rate = 0.05
decay_rate = 0.01

def gelu_pair(preact):
    tanh_arg = 0.7978845608028654 * (preact + 0.044715 * preact * preact * preact)
    tanh_val = jnp.tanh(tanh_arg)
    activation = 0.5 * preact * (1.0 + tanh_val)
    slopes = 0.5 * (1.0 + tanh_val) + 0.5 * preact * (1.0 - tanh_val * tanh_val) * 0.7978845608028654 * (1.0 + 3.0 * 0.044715 * preact * preact)
    return (activation, slopes)

def distill_target(clean, noise, teacher_first, teacher_second, step_index, teacher_count):
    steps_float = teacher_count.astype(jnp.float32)[:, None, None]
    doubled = 2.0 * step_index.astype(jnp.float32)[:, None, None]
    quarter_turn = 0.5 * math.pi
    time_now = doubled / steps_float
    time_mid = (doubled - 1.0) / steps_float
    time_end = (doubled - 2.0) / steps_float
    alpha_now = jnp.cos(quarter_turn * time_now)
    sigma_now = jnp.sin(quarter_turn * time_now)
    alpha_mid = jnp.cos(quarter_turn * time_mid)
    sigma_mid = jnp.sin(quarter_turn * time_mid)
    alpha_end = jnp.cos(quarter_turn * time_end)
    sigma_end = jnp.sin(quarter_turn * time_end)
    first_f = teacher_first.astype(jnp.float32)
    second_f = teacher_second.astype(jnp.float32)
    latent_now = alpha_now * clean.astype(jnp.float32) + sigma_now * noise.astype(jnp.float32)
    noise_now = (latent_now - alpha_now * first_f) / sigma_now
    latent_mid = alpha_mid * first_f + sigma_mid * noise_now
    noise_mid = (latent_mid - alpha_mid * second_f) / sigma_mid
    latent_end = alpha_end * second_f + sigma_end * noise_mid
    sigma_ratio = sigma_end / sigma_now
    target = (latent_end - sigma_ratio * latent_now) / (alpha_end - sigma_ratio * alpha_now)
    weighting = jnp.maximum(alpha_now * alpha_now / (sigma_now * sigma_now), 1.0)[:, 0, 0]
    return (latent_now, target, weighting)

def adam_update(master, moment, second, gradient, factor):
    clipped = gradient * factor
    moment_new = 0.9 * moment + 0.1 * clipped
    second_new = 0.999 * second + 0.001 * clipped * clipped
    first_hat = moment_new / (1.0 - 0.9 ** adam_count)
    second_hat = second_new / (1.0 - 0.999 ** adam_count)
    master_new = master - learn_rate * (first_hat / (jnp.sqrt(second_hat) + 1e-08) + decay_rate * master)
    return (master_new, moment_new, second_new)

def reference(clean, noise, teacher_first, teacher_second, step_index, teacher_count, up_master, down_master, up_moment, down_moment, up_second, down_second):
    latent, target, weighting = distill_target(clean, noise, teacher_first, teacher_second, step_index, teacher_count)
    sample_total = clean.shape[0]
    up_bf = up_master.astype(jnp.bfloat16)
    down_bf = down_master.astype(jnp.bfloat16)
    dscale = D ** (-0.5)
    fscale = FF ** (-0.5)
    down_blocks = down_bf.reshape(D, N_MP, FF // N_MP).astype(jnp.float32)

    def per_sample(state_pair, sample_item):
        loss_acc, grad_up, grad_down = state_pair
        latent_s, target_s, weight_s = sample_item
        noisy_f = lax.optimization_barrier(latent_s.astype(jnp.bfloat16)).astype(jnp.float32)
        normed = (noisy_f * lax.rsqrt(lax.optimization_barrier(jnp.mean(noisy_f * noisy_f, axis=1, keepdims=True)) + 1e-06)).astype(jnp.bfloat16)
        preact = jnp.dot(normed, up_bf, preferred_element_type=jnp.float32) * dscale
        activation, slopes = gelu_pair(preact)
        hidden = activation.astype(jnp.bfloat16)
        hidden_blocks = hidden.reshape(TOK, N_MP, FF // N_MP).astype(jnp.float32)
        terms = jnp.einsum('tkf,dkf->ktd', hidden_blocks, down_blocks) * fscale
        terms = lax.optimization_barrier(terms.astype(jnp.bfloat16)).astype(jnp.float32)
        branch = lax.optimization_barrier(jnp.sum(terms, axis=0))
        errors = latent_s + branch - target_s
        loss_acc = loss_acc + weight_s * jnp.sum(errors * errors)
        dpred = (2.0 * weight_s / sample_total * errors).astype(jnp.bfloat16)
        back_grad = jnp.dot(dpred, down_bf, preferred_element_type=jnp.float32) * fscale
        dpre = (back_grad * slopes).astype(jnp.bfloat16)
        grad_down = grad_down + lax.dot_general(dpred, hidden, (((0,), (0,)), ((), ())), preferred_element_type=jnp.float32) * fscale
        grad_up = grad_up + lax.dot_general(normed, dpre, (((0,), (0,)), ((), ())), preferred_element_type=jnp.float32) * dscale
        return ((loss_acc, grad_up, grad_down), None)
    initial = (jnp.zeros((), jnp.float32), jnp.zeros((D, FF), jnp.float32), jnp.zeros((D, FF), jnp.float32))
    (loss_acc, grad_up, grad_down), unused = lax.scan(per_sample, initial, (latent, target, weighting))
    square_sum = jnp.sum(grad_up * grad_up) + jnp.sum(grad_down * grad_down)
    clip_limit = math.sqrt(2.0 * D * FF)
    factor = clip_limit / jnp.maximum(jnp.sqrt(square_sum), clip_limit)
    new_up, up_m, up_v = adam_update(up_master, up_moment, up_second, grad_up, factor)
    new_down, down_m, down_v = adam_update(down_master, down_moment, down_second, grad_down, factor)
    loss_mean = loss_acc / (sample_total * TOK * D)
    return (new_up, new_down, up_m, down_m, up_v, down_v, loss_mean)
```

```python
import math

import jax
import jax.numpy as jnp
from jax import lax
from jax.sharding import Mesh
from jax.sharding import PartitionSpec as P

DP = ("y", "x", "c")
DP_MP = ("y", "x", "c", "mp")


adam_count = 100.0
learn_rate = 0.05
decay_rate = 0.01


def shifted(block, axis, step):
    size = lax.axis_size(axis)
    return lax.ppermute(block, axis, [(i, (i + step) % size) for i in range(size)])


def picked(blocks, index):
    return lax.dynamic_index_in_dim(blocks, index, 0, keepdims=False)


def gather_ring(block, axis):
    size = lax.axis_size(axis)
    here = lax.axis_index(axis)
    result = jnp.zeros((size,) + block.shape, block.dtype)
    for step in range(size):
        part = shifted(block, axis, step) if step else block
        result = lax.dynamic_update_index_in_dim(result, part, (here - step) % size, 0)
    return result


def scatter_ring(blocks, axis):
    size = lax.axis_size(axis)
    here = lax.axis_index(axis)
    total = picked(blocks, here)
    for step in range(1, size):
        sent = picked(blocks, (here + step) % size).astype(jnp.bfloat16)
        total = total + shifted(sent, axis, step).astype(jnp.float32)
    return total


def core_joined(blocks, rows_all):
    other = shifted(blocks, "c", 1)
    first = lax.axis_index("c") == 0
    pair = jnp.where(first, jnp.stack([blocks, other], 2), jnp.stack([other, blocks], 2))
    return pair.reshape(rows_all, blocks.shape[-1])


def gathered_weights(up_rows, down_rows):
    rows_all = up_rows.shape[0] * lax.axis_size(DP)
    ups = gather_ring(up_rows, "y")
    downs = gather_ring(down_rows, "x")
    ups = jnp.swapaxes(gather_ring(ups, "x"), 0, 1)
    downs = gather_ring(downs, "y")
    return core_joined(ups, rows_all), core_joined(downs, rows_all)


def core_summed(gradient):
    sizes = tuple(lax.axis_size(a) for a in DP)
    rows = gradient.shape[0] // math.prod(sizes)
    core = lax.axis_index("c")
    split = gradient.reshape(sizes[0] * sizes[1], 2, rows, -1)
    sent = lax.dynamic_index_in_dim(split, 1 - core, 1, keepdims=False).astype(jnp.bfloat16)
    kept = lax.dynamic_index_in_dim(split, core, 1, keepdims=False)
    return (kept + shifted(sent, "c", 1).astype(jnp.float32)).reshape(
        sizes[0], sizes[1], rows, -1
    )


def owned_up(gradient):
    blocks = jnp.swapaxes(core_summed(gradient), 0, 1)
    return scatter_ring(scatter_ring(blocks, "x"), "y")


def owned_down(gradient):
    return scatter_ring(scatter_ring(core_summed(gradient), "y"), "x")


def totals(values):
    devices = lax.axis_size(DP_MP)
    row = jnp.zeros((1, 128), jnp.float32)
    for at, value in enumerate(values):
        row = row.at[0, at].set(value)
    rows = lax.all_to_all(
        jnp.broadcast_to(row, (devices, 128)), DP_MP, split_axis=0, concat_axis=0, tiled=True
    )
    summed = jnp.sum(rows, axis=0)
    return tuple(summed[at] for at in range(len(values)))


def gelu_pair(preact):
    tanh_arg = 0.7978845608028654 * (preact + 0.044715 * preact * preact * preact)
    tanh_val = jnp.tanh(tanh_arg)
    activation = 0.5 * preact * (1.0 + tanh_val)
    slopes = 0.5 * (1.0 + tanh_val) + 0.5 * preact * (
        1.0 - tanh_val * tanh_val
    ) * 0.7978845608028654 * (1.0 + 3.0 * 0.044715 * preact * preact)
    return (activation, slopes)


def distill_target(clean, noise, teacher_first, teacher_second, step_index, teacher_count):
    steps_float = teacher_count.astype(jnp.float32)[:, None, None]
    doubled = 2.0 * step_index.astype(jnp.float32)[:, None, None]
    quarter_turn = 0.5 * math.pi
    time_now = doubled / steps_float
    time_mid = (doubled - 1.0) / steps_float
    time_end = (doubled - 2.0) / steps_float
    alpha_now = jnp.cos(quarter_turn * time_now)
    sigma_now = jnp.sin(quarter_turn * time_now)
    alpha_mid = jnp.cos(quarter_turn * time_mid)
    sigma_mid = jnp.sin(quarter_turn * time_mid)
    alpha_end = jnp.cos(quarter_turn * time_end)
    sigma_end = jnp.sin(quarter_turn * time_end)
    first_f = teacher_first.astype(jnp.float32)
    second_f = teacher_second.astype(jnp.float32)
    latent_now = alpha_now * clean.astype(jnp.float32) + sigma_now * noise.astype(jnp.float32)
    noise_now = (latent_now - alpha_now * first_f) / sigma_now
    latent_mid = alpha_mid * first_f + sigma_mid * noise_now
    noise_mid = (latent_mid - alpha_mid * second_f) / sigma_mid
    latent_end = alpha_end * second_f + sigma_end * noise_mid
    sigma_ratio = sigma_end / sigma_now
    target = (latent_end - sigma_ratio * latent_now) / (alpha_end - sigma_ratio * alpha_now)
    weighting = jnp.maximum(alpha_now * alpha_now / (sigma_now * sigma_now), 1.0)[:, 0, 0]
    return (latent_now, target, weighting)


def adam_update(master, moment, second, gradient, factor):
    clipped = gradient * factor
    moment_new = 0.9 * moment + 0.1 * clipped
    second_new = 0.999 * second + 0.001 * clipped * clipped
    first_hat = moment_new / (1.0 - 0.9**adam_count)
    second_hat = second_new / (1.0 - 0.999**adam_count)
    master_new = master - learn_rate * (
        first_hat / (jnp.sqrt(second_hat) + 1e-08) + decay_rate * master
    )
    return (master_new, moment_new, second_new)


def per_device(
    clean,
    noise,
    teacher_first,
    teacher_second,
    step_index,
    teacher_count,
    up_master,
    down_master,
    up_moment,
    down_moment,
    up_second,
    down_second,
):
    samples_dev, token_count, width_local = clean.shape
    sample_total = samples_dev * lax.axis_size(DP)
    row_count = samples_dev * token_count
    latent, target, weighting = distill_target(
        clean, noise, teacher_first, teacher_second, step_index, teacher_count
    )
    noisy_rows = latent.reshape(row_count, width_local).astype(jnp.bfloat16)
    gathered = lax.all_gather(noisy_rows, "mp", axis=1, tiled=True)
    gathered_f = gathered.astype(jnp.float32)
    normed = (
        gathered_f * lax.rsqrt(jnp.mean(gathered_f * gathered_f, axis=1, keepdims=True) + 1e-06)
    ).astype(jnp.bfloat16)
    up_full, down_full = gathered_weights(
        up_master.astype(jnp.bfloat16), down_master.astype(jnp.bfloat16)
    )
    width_full = up_full.shape[0]
    hidden_local = up_full.shape[1]
    dscale = width_full ** (-0.5)
    fscale = (hidden_local * lax.axis_size("mp")) ** (-0.5)
    preact = jnp.dot(normed, up_full, preferred_element_type=jnp.float32) * dscale
    activation, slopes = gelu_pair(preact)
    hidden = activation.astype(jnp.bfloat16)
    partial_value = (
        lax.dot_general(
            hidden, down_full, (((1,), (1,)), ((), ())), preferred_element_type=jnp.float32
        )
        * fscale
    )
    branch = lax.psum_scatter(
        partial_value.astype(jnp.bfloat16), "mp", scatter_dimension=1, tiled=True
    ).astype(jnp.float32)
    errors = latent + branch.reshape(latent.shape) - target
    weight_cube = weighting[:, None, None]
    loss_part = jnp.sum(weight_cube * errors * errors)
    dpred = (
        (2.0 * weight_cube / sample_total * errors)
        .astype(jnp.bfloat16)
        .reshape(row_count, width_local)
    )
    piece = lax.all_gather(dpred, "mp", axis=1, tiled=True)
    summed = jnp.dot(piece, down_full, preferred_element_type=jnp.float32)
    grad_piece = (
        lax.dot_general(piece, hidden, (((0,), (0,)), ((), ())), preferred_element_type=jnp.float32)
        * fscale
    )
    dpre = (summed * fscale * slopes).astype(jnp.bfloat16)
    grad_up = (
        lax.dot_general(normed, dpre, (((0,), (0,)), ((), ())), preferred_element_type=jnp.float32)
        * dscale
    )
    mine_up, mine_down = owned_up(grad_up), owned_down(grad_piece)
    squares = jnp.sum(mine_up * mine_up) + jnp.sum(mine_down * mine_down)
    loss_total, square_total = totals((loss_part, squares))
    clip_limit = math.sqrt(2.0 * width_full * hidden_local * lax.axis_size("mp"))
    factor = clip_limit / jnp.maximum(jnp.sqrt(square_total), clip_limit)
    new_up, up_m, up_v = adam_update(up_master, up_moment, up_second, mine_up, factor)
    new_down, down_m, down_v = adam_update(
        down_master, down_moment, down_second, mine_down, factor
    )
    loss_mean = loss_total / (sample_total * token_count * width_full)
    return (new_up, new_down, up_m, down_m, up_v, down_v, loss_mean)


def solution(mesh):
    split = Mesh(mesh.devices.reshape(4, 4, 2, mesh.shape["mp"]), DP_MP)
    placed = (
        P(DP, None, "mp"),
        P(DP, None, "mp"),
        P(DP, None, "mp"),
        P(DP, None, "mp"),
        P(DP),
        P(DP),
        P(DP, "mp"),
        P(DP, "mp"),
        P(DP, "mp"),
        P(DP, "mp"),
        P(DP, "mp"),
        P(DP, "mp"),
    )
    return jax.shard_map(
        per_device,
        mesh=split,
        in_specs=placed,
        out_specs=(
            P(DP, "mp"),
            P(DP, "mp"),
            P(DP, "mp"),
            P(DP, "mp"),
            P(DP, "mp"),
            P(DP, "mp"),
            P(),
        ),
        check_vma=False,
    )
```

```python
import math

import jax
import jax.numpy as jnp
from jax import lax
from jax.sharding import Mesh
from jax.sharding import PartitionSpec as P


DP = ("y", "x", "c")
DP_MP = ("y", "x", "c", "mp")


adam_count = 100.0
learn_rate = 0.05
decay_rate = 0.01


PLANE = ("y", "x")


def core_swapped(block):
    return lax.ppermute(block, "c", [(0, 1), (1, 0)])


def core_joined(mine, other):
    first = lax.axis_index("c") == 0
    pair = jnp.where(first, jnp.stack([mine, other], 1), jnp.stack([other, mine], 1))
    return pair.reshape(-1, mine.shape[-1])


def gathered_weights(up_rows, down_rows):
    chips = lax.axis_size(PLANE)
    rows = up_rows.shape[0]
    both = jnp.concatenate([up_rows, down_rows], axis=0)
    mine = lax.all_to_all(
        jnp.broadcast_to(both, (chips,) + both.shape), PLANE, split_axis=0, concat_axis=0, tiled=True
    )
    other = core_swapped(mine)
    return (
        core_joined(mine[:, :rows], other[:, :rows]),
        core_joined(mine[:, rows:], other[:, rows:]),
    )


def core_split(gradient):
    rows = gradient.shape[0] // lax.axis_size(DP)
    core = lax.axis_index("c")
    split = gradient.reshape(lax.axis_size(PLANE), 2, rows, -1)
    sent = lax.dynamic_index_in_dim(split, 1 - core, 1, keepdims=False).astype(jnp.bfloat16)
    return sent, lax.dynamic_index_in_dim(split, core, 1, keepdims=False)


def chip_added(kept, other):
    return (kept + other.astype(jnp.float32)).astype(jnp.bfloat16)


def plane_parts(chip_sum):
    return lax.all_to_all(chip_sum, PLANE, split_axis=0, concat_axis=0, tiled=True)


def added(parts):
    return jnp.sum(parts.astype(jnp.float32), axis=0)


def totals(values):
    devices = lax.axis_size(DP_MP)
    row = jnp.zeros((1, 128), jnp.float32)
    for at, value in enumerate(values):
        row = row.at[0, at].set(value)
    rows = lax.all_to_all(
        jnp.broadcast_to(row, (devices, 128)), DP_MP, split_axis=0, concat_axis=0, tiled=True
    )
    summed = jnp.sum(rows, axis=0)
    return tuple(summed[at] for at in range(len(values)))


def gelu_pair(preact):
    tanh_arg = 0.7978845608028654 * (preact + 0.044715 * preact * preact * preact)
    tanh_val = jnp.tanh(tanh_arg)
    activation = 0.5 * preact * (1.0 + tanh_val)
    slopes = 0.5 * (1.0 + tanh_val) + 0.5 * preact * (
        1.0 - tanh_val * tanh_val
    ) * 0.7978845608028654 * (1.0 + 3.0 * 0.044715 * preact * preact)
    return (activation, slopes)


def distill_target(clean, noise, teacher_first, teacher_second, step_index, teacher_count):
    steps_float = teacher_count.astype(jnp.float32)[:, None, None]
    doubled = 2.0 * step_index.astype(jnp.float32)[:, None, None]
    quarter_turn = 0.5 * math.pi
    time_now = doubled / steps_float
    time_mid = (doubled - 1.0) / steps_float
    time_end = (doubled - 2.0) / steps_float
    alpha_now = jnp.cos(quarter_turn * time_now)
    sigma_now = jnp.sin(quarter_turn * time_now)
    alpha_mid = jnp.cos(quarter_turn * time_mid)
    sigma_mid = jnp.sin(quarter_turn * time_mid)
    alpha_end = jnp.cos(quarter_turn * time_end)
    sigma_end = jnp.sin(quarter_turn * time_end)
    first_f = teacher_first.astype(jnp.float32)
    second_f = teacher_second.astype(jnp.float32)
    latent_now = alpha_now * clean.astype(jnp.float32) + sigma_now * noise.astype(jnp.float32)
    noise_now = (latent_now - alpha_now * first_f) / sigma_now
    latent_mid = alpha_mid * first_f + sigma_mid * noise_now
    noise_mid = (latent_mid - alpha_mid * second_f) / sigma_mid
    latent_end = alpha_end * second_f + sigma_end * noise_mid
    sigma_ratio = sigma_end / sigma_now
    target = (latent_end - sigma_ratio * latent_now) / (alpha_end - sigma_ratio * alpha_now)
    weighting = jnp.maximum(alpha_now * alpha_now / (sigma_now * sigma_now), 1.0)[:, 0, 0]
    return (latent_now, target, weighting)


def adam_update(master, moment, second, gradient, factor):
    clipped = gradient * factor
    moment_new = 0.9 * moment + 0.1 * clipped
    second_new = 0.999 * second + 0.001 * clipped * clipped
    first_hat = moment_new / (1.0 - 0.9**adam_count)
    second_hat = second_new / (1.0 - 0.999**adam_count)
    master_new = master - learn_rate * (
        first_hat / (jnp.sqrt(second_hat) + 1e-08) + decay_rate * master
    )
    return (master_new, moment_new, second_new)


def per_device(
    clean,
    noise,
    teacher_first,
    teacher_second,
    step_index,
    teacher_count,
    up_master,
    down_master,
    up_moment,
    down_moment,
    up_second,
    down_second,
):
    samples_dev, token_count, width_local = clean.shape
    sample_total = samples_dev * lax.axis_size(DP)
    row_count = samples_dev * token_count
    latent, target, weighting = distill_target(
        clean, noise, teacher_first, teacher_second, step_index, teacher_count
    )
    noisy_rows = latent.reshape(row_count, width_local).astype(jnp.bfloat16)
    gathered = lax.all_gather(noisy_rows, "mp", axis=1, tiled=True)
    gathered_f = gathered.astype(jnp.float32)
    normed = (
        gathered_f * lax.rsqrt(jnp.mean(gathered_f * gathered_f, axis=1, keepdims=True) + 1e-06)
    ).astype(jnp.bfloat16)
    up_full, down_full = gathered_weights(
        up_master.astype(jnp.bfloat16), down_master.astype(jnp.bfloat16)
    )
    width_full = up_full.shape[0]
    hidden_local = up_full.shape[1]
    dscale = width_full ** (-0.5)
    fscale = (hidden_local * lax.axis_size("mp")) ** (-0.5)
    preact = jnp.dot(normed, up_full, preferred_element_type=jnp.float32) * dscale
    activation, slopes = gelu_pair(preact)
    hidden = activation.astype(jnp.bfloat16)
    partial_value = (
        lax.dot_general(
            hidden, down_full, (((1,), (1,)), ((), ())), preferred_element_type=jnp.float32
        )
        * fscale
    )
    branch = lax.psum_scatter(
        partial_value.astype(jnp.bfloat16), "mp", scatter_dimension=1, tiled=True
    ).astype(jnp.float32)
    errors = latent + branch.reshape(latent.shape) - target
    weight_cube = weighting[:, None, None]
    loss_part = jnp.sum(weight_cube * errors * errors)
    dpred = (
        (2.0 * weight_cube / sample_total * errors)
        .astype(jnp.bfloat16)
        .reshape(row_count, width_local)
    )
    piece = lax.all_gather(dpred, "mp", axis=1, tiled=True)
    grad_piece = (
        lax.dot_general(piece, hidden, (((0,), (0,)), ((), ())), preferred_element_type=jnp.float32)
        * fscale
    )
    sent_down, kept_down = core_split(grad_piece)
    other_down = core_swapped(sent_down)
    piece, sent_down = lax.optimization_barrier((piece, sent_down))
    summed = jnp.dot(piece, down_full, preferred_element_type=jnp.float32)
    dpre = (summed * fscale * slopes).astype(jnp.bfloat16)
    dpre, chip_down = lax.optimization_barrier((dpre, chip_added(kept_down, other_down)))
    parts_down = plane_parts(chip_down)
    grad_up = (
        lax.dot_general(normed, dpre, (((0,), (0,)), ((), ())), preferred_element_type=jnp.float32)
        * dscale
    )
    sent_up, kept_up = core_split(grad_up)
    parts_up = plane_parts(chip_added(kept_up, core_swapped(sent_up)))
    mine_up, mine_down = added(parts_up), added(parts_down)
    squares = jnp.sum(mine_up * mine_up) + jnp.sum(mine_down * mine_down)
    loss_total, square_total = totals((loss_part, squares))
    clip_limit = math.sqrt(2.0 * width_full * hidden_local * lax.axis_size("mp"))
    factor = clip_limit / jnp.maximum(jnp.sqrt(square_total), clip_limit)
    new_up, up_m, up_v = adam_update(up_master, up_moment, up_second, mine_up, factor)
    new_down, down_m, down_v = adam_update(
        down_master, down_moment, down_second, mine_down, factor
    )
    loss_mean = loss_total / (sample_total * token_count * width_full)
    return (new_up, new_down, up_m, down_m, up_v, down_v, loss_mean)


def solution(mesh):
    split = Mesh(mesh.devices.reshape(4, 4, 2, mesh.shape["mp"]), DP_MP)
    placed = (
        P(DP, None, "mp"),
        P(DP, None, "mp"),
        P(DP, None, "mp"),
        P(DP, None, "mp"),
        P(DP),
        P(DP),
        P(DP, "mp"),
        P(DP, "mp"),
        P(DP, "mp"),
        P(DP, "mp"),
        P(DP, "mp"),
        P(DP, "mp"),
    )

    return jax.shard_map(
        per_device,
        mesh=split,
        in_specs=placed,
        out_specs=(
            P(DP, "mp"),
            P(DP, "mp"),
            P(DP, "mp"),
            P(DP, "mp"),
            P(DP, "mp"),
            P(DP, "mp"),
            P(),
        ),
        check_vma=False,
    )
```

```python
import math

import jax
import jax.numpy as jnp
from jax import lax
from jax.sharding import Mesh
from jax.sharding import PartitionSpec as P

DP = ("y", "x", "c")
DP_MP = ("y", "x", "c", "mp")


adam_count = 100.0
learn_rate = 0.05
decay_rate = 0.01


PLANE = ("y", "x")


def core_swapped(block):
    return lax.ppermute(block, "c", [(0, 1), (1, 0)])


def core_joined(mine, other):
    first = lax.axis_index("c") == 0
    pair = jnp.where(first, jnp.stack([mine, other], 1), jnp.stack([other, mine], 1))
    return pair.reshape(-1, mine.shape[-1])


def gathered_weights(up_rows, down_rows):
    chips = lax.axis_size(PLANE)
    rows = up_rows.shape[0]
    both = jnp.concatenate([up_rows, down_rows], axis=0)
    mine = lax.all_to_all(
        jnp.broadcast_to(both, (chips,) + both.shape), PLANE, split_axis=0, concat_axis=0, tiled=True
    )
    other = core_swapped(mine)
    return (
        core_joined(mine[:, :rows], other[:, :rows]),
        core_joined(mine[:, rows:], other[:, rows:]),
    )


def half_columns(block, which):
    half = block.shape[1] // 2
    return lax.dynamic_slice_in_dim(block, which * half, half, axis=1)


def over_tokens(left, right):
    return lax.dot_general(left, right, (((0,), (0,)), ((), ())), preferred_element_type=jnp.float32)


def totals(first, second):
    shape = (lax.axis_size(DP_MP), 128)
    lane = lax.broadcasted_iota(jnp.int32, shape, 1)
    rows = lax.all_to_all(
        jnp.where(lane < 64, first, second), DP_MP, split_axis=0, concat_axis=0, tiled=True
    )
    summed = jnp.sum(rows, axis=0)
    return summed[0], summed[64]


def gelu_pair(preact):
    tanh_arg = 0.7978845608028654 * (preact + 0.044715 * preact * preact * preact)
    tanh_val = jnp.tanh(tanh_arg)
    activation = 0.5 * preact * (1.0 + tanh_val)
    slopes = 0.5 * (1.0 + tanh_val) + 0.5 * preact * (
        1.0 - tanh_val * tanh_val
    ) * 0.7978845608028654 * (1.0 + 3.0 * 0.044715 * preact * preact)
    return (activation, slopes)


def distill_target(clean, noise, teacher_first, teacher_second, step_index, teacher_count):
    steps_float = teacher_count.astype(jnp.float32)[:, None, None]
    doubled = 2.0 * step_index.astype(jnp.float32)[:, None, None]
    quarter_turn = 0.5 * math.pi
    time_now = doubled / steps_float
    time_mid = (doubled - 1.0) / steps_float
    time_end = (doubled - 2.0) / steps_float
    alpha_now = jnp.cos(quarter_turn * time_now)
    sigma_now = jnp.sin(quarter_turn * time_now)
    alpha_mid = jnp.cos(quarter_turn * time_mid)
    sigma_mid = jnp.sin(quarter_turn * time_mid)
    alpha_end = jnp.cos(quarter_turn * time_end)
    sigma_end = jnp.sin(quarter_turn * time_end)
    first_f = teacher_first.astype(jnp.float32)
    second_f = teacher_second.astype(jnp.float32)
    latent_now = alpha_now * clean.astype(jnp.float32) + sigma_now * noise.astype(jnp.float32)
    noise_now = (latent_now - alpha_now * first_f) / sigma_now
    latent_mid = alpha_mid * first_f + sigma_mid * noise_now
    noise_mid = (latent_mid - alpha_mid * second_f) / sigma_mid
    latent_end = alpha_end * second_f + sigma_end * noise_mid
    sigma_ratio = sigma_end / sigma_now
    target = (latent_end - sigma_ratio * latent_now) / (alpha_end - sigma_ratio * alpha_now)
    weighting = jnp.maximum(alpha_now * alpha_now / (sigma_now * sigma_now), 1.0)[:, 0, 0]
    return (latent_now, target, weighting)


def adam_update(master, moment, second, gradient, factor):
    clipped = gradient * factor
    moment_new = 0.9 * moment + 0.1 * clipped
    second_new = 0.999 * second + 0.001 * clipped * clipped
    first_hat = moment_new / (1.0 - 0.9**adam_count)
    second_hat = second_new / (1.0 - 0.999**adam_count)
    master_new = master - learn_rate * (
        first_hat / (jnp.sqrt(second_hat) + 1e-08) + decay_rate * master
    )
    return (master_new, moment_new, second_new)


def per_device(
    clean,
    noise,
    teacher_first,
    teacher_second,
    step_index,
    teacher_count,
    up_master,
    down_master,
    up_moment,
    down_moment,
    up_second,
    down_second,
):
    samples_dev, token_count, width_local = clean.shape
    sample_total = samples_dev * lax.axis_size(DP)
    row_count = samples_dev * token_count
    latent, target, weighting = distill_target(
        clean, noise, teacher_first, teacher_second, step_index, teacher_count
    )
    noisy_rows = latent.reshape(row_count, width_local).astype(jnp.bfloat16)
    gathered = lax.all_gather(noisy_rows, "mp", axis=1, tiled=True)
    gathered_f = gathered.astype(jnp.float32)
    normed = (
        gathered_f * lax.rsqrt(jnp.mean(gathered_f * gathered_f, axis=1, keepdims=True) + 1e-06)
    ).astype(jnp.bfloat16)
    up_full, down_full = gathered_weights(
        up_master.astype(jnp.bfloat16), down_master.astype(jnp.bfloat16)
    )
    width_full = up_full.shape[0]
    hidden_local = up_full.shape[1]
    dscale = width_full ** (-0.5)
    fscale = (hidden_local * lax.axis_size("mp")) ** (-0.5)
    preact = jnp.dot(normed, up_full, preferred_element_type=jnp.float32) * dscale
    activation, slopes = gelu_pair(preact)
    hidden = activation.astype(jnp.bfloat16)
    core = lax.axis_index("c")
    partial_value = (
        lax.dot_general(
            hidden, down_full, (((1,), (1,)), ((), ())), preferred_element_type=jnp.float32
        )
        * fscale
    ).astype(jnp.bfloat16)
    offset = lax.optimization_barrier(latent - target)
    branch = lax.psum_scatter(partial_value, "mp", scatter_dimension=1, tiled=True).astype(
        jnp.float32
    )
    normed_other, hidden_other = core_swapped(normed), core_swapped(half_columns(hidden, 1 - core))
    errors = offset + branch.reshape(latent.shape)
    weight_cube = weighting[:, None, None]
    loss_part = jnp.sum(weight_cube * errors * errors)
    dpred = (
        (2.0 * weight_cube / sample_total * errors)
        .astype(jnp.bfloat16)
        .reshape(row_count, width_local)
    )
    piece = lax.all_gather(dpred, "mp", axis=1, tiled=True)
    piece_other = core_swapped(piece)
    summed = jnp.dot(piece, down_full, preferred_element_type=jnp.float32)
    dpre = (summed * fscale * slopes).astype(jnp.bfloat16)
    dpre_other = core_swapped(half_columns(dpre, 1 - core))
    grad_down = (
        over_tokens(piece, half_columns(hidden, core)) + over_tokens(piece_other, hidden_other)
    ) * fscale
    grad_up = (
        over_tokens(normed, half_columns(dpre, core)) + over_tokens(normed_other, dpre_other)
    ) * dscale
    chips = lax.axis_size(PLANE)
    rows_chip = width_full // chips
    halves = [
        g.astype(jnp.bfloat16).reshape(chips, rows_chip, -1) for g in (grad_up, grad_down)
    ]
    parts = lax.all_to_all(
        jnp.concatenate(halves, axis=1), PLANE, split_axis=0, concat_axis=0, tiled=True
    )
    chip_rows = jnp.sum(parts.astype(jnp.float32), axis=0)
    squares = jnp.sum(chip_rows * chip_rows)
    loss_total, square_total = totals(loss_part, squares)
    by_core = chip_rows.reshape(2, 2, rows_chip // 2, -1)
    kept = lax.dynamic_index_in_dim(by_core, core, 1, keepdims=False)
    other = core_swapped(lax.dynamic_index_in_dim(by_core, 1 - core, 1, keepdims=False))
    mine_up, mine_down = jnp.where(
        core == 0, jnp.concatenate([kept, other], 2), jnp.concatenate([other, kept], 2)
    )
    clip_limit = math.sqrt(2.0 * width_full * hidden_local * lax.axis_size("mp"))
    factor = clip_limit / jnp.maximum(jnp.sqrt(square_total), clip_limit)
    new_up, up_m, up_v = adam_update(up_master, up_moment, up_second, mine_up, factor)
    new_down, down_m, down_v = adam_update(
        down_master, down_moment, down_second, mine_down, factor
    )
    loss_mean = loss_total / (sample_total * token_count * width_full)
    return (new_up, new_down, up_m, down_m, up_v, down_v, loss_mean)


def solution(mesh):
    split = Mesh(mesh.devices.reshape(4, 4, 2, mesh.shape["mp"]), DP_MP)
    placed = (
        P(DP, None, "mp"),
        P(DP, None, "mp"),
        P(DP, None, "mp"),
        P(DP, None, "mp"),
        P(DP),
        P(DP),
        P(DP, "mp"),
        P(DP, "mp"),
        P(DP, "mp"),
        P(DP, "mp"),
        P(DP, "mp"),
        P(DP, "mp"),
    )

    return jax.shard_map(
        per_device,
        mesh=split,
        in_specs=placed,
        out_specs=(
            P(DP, "mp"),
            P(DP, "mp"),
            P(DP, "mp"),
            P(DP, "mp"),
            P(DP, "mp"),
            P(DP, "mp"),
            P(),
        ),
        check_vma=False,
    )
```

```python
import functools
import math

import jax
import jax.numpy as jnp
from jax import lax
from jax.experimental import pallas as pl
from jax.experimental.pallas import tpu as pltpu
from jax.sharding import Mesh
from jax.sharding import PartitionSpec as P


DP = ("y", "x", "c")
DP_MP = ("y", "x", "c", "mp")


adam_count = 100.0
learn_rate = 0.05
decay_rate = 0.01


PLANE = ("y", "x")


def core_swapped(block):
    return lax.ppermute(block, "c", [(0, 1), (1, 0)])


def core_joined(mine, other):
    first = lax.axis_index("c") == 0
    pair = jnp.where(first, jnp.stack([mine, other], 1), jnp.stack([other, mine], 1))
    return pair.reshape(-1, mine.shape[-1])


def gathered_weights(up_rows, down_rows):
    chips = lax.axis_size(PLANE)
    rows = up_rows.shape[0]
    both = jnp.concatenate([up_rows, down_rows], axis=0)
    mine = lax.all_to_all(
        jnp.broadcast_to(both, (chips,) + both.shape), PLANE, split_axis=0, concat_axis=0, tiled=True
    )
    other = core_swapped(mine)
    return (
        core_joined(mine[:, :rows], other[:, :rows]),
        core_joined(mine[:, rows:], other[:, rows:]),
    )


def half_columns(block, which):
    half = block.shape[1] // 2
    return lax.dynamic_slice_in_dim(block, which * half, half, axis=1)


def gradient_kernel(first, first_units, second, second_units, result, *, scale):
    added = jnp.dot(first[...], first_units[...], preferred_element_type=jnp.float32)
    added += jnp.dot(second[...], second_units[...], preferred_element_type=jnp.float32)
    result[...] = (added * scale).astype(result.dtype)


def weight_gradient(first, first_units, second, second_units, at, scale):
    features, tokens = first.shape
    units = first_units.shape[1]
    block = features // 6
    return pl.pallas_call(
        functools.partial(gradient_kernel, scale=scale),
        out_shape=jax.ShapeDtypeStruct((features, units), jnp.bfloat16),
        grid=(features // block,),
        in_specs=[
            pl.BlockSpec((block, tokens), lambda i: (i, 0)),
            pl.BlockSpec((tokens, units), lambda i: (0, 0)),
            pl.BlockSpec((block, tokens), lambda i: (i + at[0], 0)),
            pl.BlockSpec((tokens, units), lambda i: (0, at[1])),
        ],
        out_specs=pl.BlockSpec((block, units), lambda i: (i, 0)),
        cost_estimate=pl.CostEstimate(
            flops=4 * features * tokens * units,
            transcendentals=0,
            bytes_accessed=4 * (features + units) * tokens + 2 * features * units,
        ),
        compiler_params=pltpu.CompilerParams(dimension_semantics=("arbitrary",)),
    )(first, first_units, second, second_units)


def hidden_kernel(core, piece, down, slopes, mine, sent, *, scale):
    summed = lax.dot_general(
        piece[...], down[...], (((0,), (0,)), ((), ())), preferred_element_type=jnp.float32
    )
    rounded = (summed * scale * slopes[...]).astype(mine.dtype)
    half = mine.shape[1]
    low, high = rounded[:, :half], rounded[:, half:]

    @pl.when(core[0] == 0)
    def _():
        mine[...] = low
        sent[...] = high

    @pl.when(core[0] != 0)
    def _():
        mine[...] = high
        sent[...] = low


def hidden_gradient(core, piece, down, slopes, scale):
    features, tokens = piece.shape
    units = down.shape[1]
    block = tokens // 4
    half = jax.ShapeDtypeStruct((tokens, units // 2), jnp.bfloat16)
    return pl.pallas_call(
        functools.partial(hidden_kernel, scale=scale),
        out_shape=(half, half),
        grid=(tokens // block,),
        in_specs=[
            pl.BlockSpec(memory_space=pltpu.SMEM),
            pl.BlockSpec((features, block), lambda i: (0, i)),
            pl.BlockSpec((features, units), lambda i: (0, 0)),
            pl.BlockSpec((block, units), lambda i: (i, 0)),
        ],
        out_specs=(
            pl.BlockSpec((block, units // 2), lambda i: (i, 0)),
            pl.BlockSpec((block, units // 2), lambda i: (i, 0)),
        ),
        cost_estimate=pl.CostEstimate(
            flops=2 * features * tokens * units,
            transcendentals=0,
            bytes_accessed=2 * features * (tokens + units) + 6 * tokens * units,
        ),
        compiler_params=pltpu.CompilerParams(dimension_semantics=("arbitrary",)),
        name="hidden_gradient",
    )(core.reshape(1), piece, down, slopes)


def from_plane(halves):
    parts = lax.all_to_all(halves, PLANE, split_axis=0, concat_axis=0, tiled=True)
    return jnp.sum(parts.astype(jnp.float32), axis=0)


def from_axis(blocks, axis):
    size = lax.axis_size(axis)
    here = lax.axis_index(axis)
    total = lax.dynamic_index_in_dim(blocks, here, 0, keepdims=False).astype(jnp.float32)
    for step in range(1, size):
        sent = lax.dynamic_index_in_dim(blocks, (here + step) % size, 0, keepdims=False)
        moved = lax.ppermute(
            sent.astype(jnp.bfloat16), axis, [(i, (i + step) % size) for i in range(size)]
        )
        total = total + moved.astype(jnp.float32)
    return total


def totals(first, second):
    shape = (lax.axis_size(DP_MP), 128)
    lane = lax.broadcasted_iota(jnp.int32, shape, 1)
    rows = lax.all_to_all(
        jnp.where(lane < 64, first, second), DP_MP, split_axis=0, concat_axis=0, tiled=True
    )
    summed = jnp.sum(rows, axis=0)
    return summed[0], summed[64]


def over_features(left, right):
    return lax.dot_general(left, right, (((0,), (0,)), ((), ())), preferred_element_type=jnp.float32)


def gelu_pair(preact):
    tanh_arg = 0.7978845608028654 * (preact + 0.044715 * preact * preact * preact)
    tanh_val = jnp.tanh(tanh_arg)
    activation = 0.5 * preact * (1.0 + tanh_val)
    slopes = 0.5 * (1.0 + tanh_val) + 0.5 * preact * (
        1.0 - tanh_val * tanh_val
    ) * 0.7978845608028654 * (1.0 + 3.0 * 0.044715 * preact * preact)
    return (activation, slopes)


def rates(step_index, teacher_count):
    steps_float = teacher_count.astype(jnp.float32)
    doubled = 2.0 * step_index.astype(jnp.float32)
    back = jnp.arange(3, dtype=jnp.float32)[:, None]
    angles = 0.5 * math.pi * ((doubled - back) / steps_float)
    return jnp.cos(angles)[:, :, None, None], jnp.sin(angles)[:, :, None, None]


def noisy_latent(clean, noise, alphas, sigmas):
    return alphas[0] * clean.astype(jnp.float32) + sigmas[0] * noise.astype(jnp.float32)


def distill_target(latent_now, teacher_first, teacher_second, alphas, sigmas):
    alpha_now, alpha_mid, alpha_end = alphas
    sigma_now, sigma_mid, sigma_end = sigmas
    first_f = teacher_first.astype(jnp.float32)
    second_f = teacher_second.astype(jnp.float32)
    noise_now = (latent_now - alpha_now * first_f) / sigma_now
    latent_mid = alpha_mid * first_f + sigma_mid * noise_now
    noise_mid = (latent_mid - alpha_mid * second_f) / sigma_mid
    latent_end = alpha_end * second_f + sigma_end * noise_mid
    sigma_ratio = sigma_end / sigma_now
    return (latent_end - sigma_ratio * latent_now) / (alpha_end - sigma_ratio * alpha_now)


def adam_update(master, moment, second, gradient, factor):
    clipped = gradient * factor
    moment_new = 0.9 * moment + 0.1 * clipped
    second_new = 0.999 * second + 0.001 * clipped * clipped
    first_hat = moment_new / (1.0 - 0.9**adam_count)
    second_hat = second_new / (1.0 - 0.999**adam_count)
    master_new = master - learn_rate * (
        first_hat / (jnp.sqrt(second_hat) + 1e-08) + decay_rate * master
    )
    return (master_new, moment_new, second_new)


def per_device(
    clean,
    noise,
    teacher_first,
    teacher_second,
    step_index,
    teacher_count,
    up_master,
    down_master,
    up_moment,
    down_moment,
    up_second,
    down_second,
):
    samples_dev, token_count, width_local = clean.shape
    sample_total = samples_dev * lax.axis_size(DP)
    row_count = samples_dev * token_count
    alphas, sigmas = rates(step_index, teacher_count)
    weighting = jnp.maximum(alphas[0] * alphas[0] / (sigmas[0] * sigmas[0]), 1.0)
    latent = noisy_latent(clean, noise, alphas, sigmas)
    noisy_rows = latent.reshape(row_count, width_local).astype(jnp.bfloat16)
    gathered = lax.all_gather(noisy_rows.T, "mp", axis=0, tiled=True)
    *held, gathered = lax.optimization_barrier(
        (clean, noise, teacher_first, teacher_second, gathered)
    )
    latent_again = noisy_latent(*held[:2], alphas, sigmas)
    target = distill_target(latent_again, *held[2:], alphas, sigmas)
    offset = latent_again - target
    gathered_f = gathered.astype(jnp.float32)
    normed = (
        gathered_f * lax.rsqrt(jnp.mean(gathered_f * gathered_f, axis=0, keepdims=True) + 1e-06)
    ).astype(jnp.bfloat16)
    up_full, down_full = gathered_weights(
        up_master.astype(jnp.bfloat16), down_master.astype(jnp.bfloat16)
    )
    width_full = up_full.shape[0]
    hidden_local = up_full.shape[1]
    dscale = width_full ** (-0.5)
    fscale = (hidden_local * lax.axis_size("mp")) ** (-0.5)
    preact = over_features(normed, up_full) * dscale
    activation, slopes = gelu_pair(preact)
    hidden = activation.astype(jnp.bfloat16)
    core = lax.axis_index("c")
    partial_value = (
        lax.dot_general(
            down_full, hidden, (((1,), (1,)), ((), ())), preferred_element_type=jnp.float32
        )
        * fscale
    ).astype(jnp.bfloat16)
    branch = lax.psum_scatter(partial_value, "mp", scatter_dimension=0, tiled=True).astype(
        jnp.float32
    )
    offset, normed_other, hidden_mine, hidden_other = lax.optimization_barrier(
        (
            offset,
            core_swapped(normed),
            half_columns(hidden, core),
            core_swapped(half_columns(hidden, 1 - core)),
        )
    )
    errors = offset + branch.T.reshape(latent.shape)
    weight_cube = weighting
    loss_part = jnp.sum(weight_cube * errors * errors)
    dpred = (
        (2.0 * weight_cube / sample_total * errors)
        .astype(jnp.bfloat16)
        .reshape(row_count, width_local)
    )
    piece = lax.all_gather(dpred.T, "mp", axis=0, tiled=True)
    piece_other = core_swapped(piece)
    dpre_mine, dpre_sent = hidden_gradient(core, piece, down_full, slopes, fscale)
    dpre_other = core_swapped(dpre_sent)
    grad_down = weight_gradient(piece, hidden_mine, piece_other, hidden_other, (0, 0), fscale)
    grad_up = weight_gradient(normed, dpre_mine, normed_other, dpre_other, (0, 0), dscale)
    chips = lax.axis_size(PLANE)
    rows_chip = width_full // chips
    rows_down = from_plane(grad_down.reshape(chips, rows_chip, -1))
    blocks_up = grad_up.reshape(
        lax.axis_size("y"), lax.axis_size("x"), rows_chip, -1
    )
    rows_up = from_axis(from_axis(jnp.swapaxes(blocks_up, 0, 1), "x"), "y")
    chip_rows = jnp.stack([rows_up, rows_down])
    squares = jnp.sum(chip_rows * chip_rows)
    loss_total, square_total = totals(loss_part, squares)
    by_core = chip_rows.reshape(2, 2, rows_chip // 2, -1)
    kept = lax.dynamic_index_in_dim(by_core, core, 1, keepdims=False)
    other = core_swapped(lax.dynamic_index_in_dim(by_core, 1 - core, 1, keepdims=False))
    mine_up, mine_down = jnp.where(
        core == 0, jnp.concatenate([kept, other], 2), jnp.concatenate([other, kept], 2)
    )
    clip_limit = math.sqrt(2.0 * width_full * hidden_local * lax.axis_size("mp"))
    factor = clip_limit / jnp.maximum(jnp.sqrt(square_total), clip_limit)
    new_up, up_m, up_v = adam_update(up_master, up_moment, up_second, mine_up, factor)
    new_down, down_m, down_v = adam_update(
        down_master, down_moment, down_second, mine_down, factor
    )
    loss_mean = loss_total / (sample_total * token_count * width_full)
    return (new_up, new_down, up_m, down_m, up_v, down_v, loss_mean)


def solution(mesh):
    split = Mesh(mesh.devices.reshape(4, 4, 2, mesh.shape["mp"]), DP_MP)
    placed = (
        P(DP, None, "mp"),
        P(DP, None, "mp"),
        P(DP, None, "mp"),
        P(DP, None, "mp"),
        P(DP),
        P(DP),
        P(DP, "mp"),
        P(DP, "mp"),
        P(DP, "mp"),
        P(DP, "mp"),
        P(DP, "mp"),
        P(DP, "mp"),
    )

    return jax.shard_map(
        per_device,
        mesh=split,
        in_specs=placed,
        out_specs=(
            P(DP, "mp"),
            P(DP, "mp"),
            P(DP, "mp"),
            P(DP, "mp"),
            P(DP, "mp"),
            P(DP, "mp"),
            P(),
        ),
        check_vma=False,
    )
```

```python
import functools
import math

import jax
import jax.numpy as jnp
from jax import lax
from jax.experimental import pallas as pl
from jax.experimental.pallas import tpu as pltpu
from jax.sharding import Mesh
from jax.sharding import PartitionSpec as P


DP = ("y", "x", "c")
DP_MP = ("y", "x", "c", "mp")


adam_count = 100.0
learn_rate = 0.05
decay_rate = 0.01


PLANE = ("y", "x")


def core_swapped(block):
    return lax.ppermute(block, "c", [(0, 1), (1, 0)])


def core_joined(mine, other):
    first = lax.axis_index("c") == 0
    pair = jnp.where(first, jnp.stack([mine, other], 1), jnp.stack([other, mine], 1))
    return pair.reshape(-1, mine.shape[-1])


def gathered_weights(up_rows, down_rows):
    chips = lax.axis_size(PLANE)
    rows = up_rows.shape[0]
    both = jnp.concatenate([up_rows, down_rows], axis=0)
    mine = lax.all_to_all(
        jnp.broadcast_to(both, (chips,) + both.shape), PLANE, split_axis=0, concat_axis=0, tiled=True
    )
    other = core_swapped(mine)
    return (
        core_joined(mine[:, :rows], other[:, :rows]),
        core_joined(mine[:, rows:], other[:, rows:]),
    )


def halves_kept(core, block, mine, sent):
    half = mine.shape[1]

    @pl.when(core == 0)
    def _():
        mine[...] = block[:, :half]
        sent[...] = block[:, half:]

    @pl.when(core != 0)
    def _():
        mine[...] = block[:, half:]
        sent[...] = block[:, :half]


def forward_kernel(core, gathered, up, down, normed, mine, sent, slopes, partial, *, up_scale, down_scale):
    tokens = gathered[...].astype(jnp.float32)
    mean = jnp.mean(tokens * tokens, axis=0, keepdims=True)
    rounded = (tokens * lax.rsqrt(mean + 1e-06)).astype(normed.dtype)
    normed[...] = rounded
    preact = over_features(rounded, up[...]) * up_scale
    activation, slope = gelu_pair(preact)
    slopes[...] = slope
    hidden = activation.astype(mine.dtype)
    halves_kept(core[0], hidden, mine, sent)
    summed = lax.dot_general(
        down[...], hidden, (((1,), (1,)), ((), ())), preferred_element_type=jnp.float32
    )
    partial[...] = (summed * down_scale).astype(partial.dtype)


def forward(core, gathered, up, down, up_scale, down_scale):
    features, tokens = gathered.shape
    units = up.shape[1]
    block = tokens // 4
    by_feature = pl.BlockSpec((features, block), lambda i: (0, i))
    by_half = pl.BlockSpec((block, units // 2), lambda i: (i, 0))
    whole = pl.BlockSpec((features, units), lambda i: (0, 0))
    return pl.pallas_call(
        functools.partial(forward_kernel, up_scale=up_scale, down_scale=down_scale),
        out_shape=(
            jax.ShapeDtypeStruct((features, tokens), jnp.bfloat16),
            jax.ShapeDtypeStruct((tokens, units // 2), jnp.bfloat16),
            jax.ShapeDtypeStruct((tokens, units // 2), jnp.bfloat16),
            jax.ShapeDtypeStruct((tokens, units), jnp.float32),
            jax.ShapeDtypeStruct((features, tokens), jnp.bfloat16),
        ),
        grid=(tokens // block,),
        in_specs=[pl.BlockSpec(memory_space=pltpu.SMEM), by_feature, whole, whole],
        out_specs=(
            by_feature,
            by_half,
            by_half,
            pl.BlockSpec((block, units), lambda i: (i, 0)),
            by_feature,
        ),
        cost_estimate=pl.CostEstimate(
            flops=4 * features * tokens * units,
            transcendentals=tokens * units,
            bytes_accessed=6 * features * tokens + 4 * features * units + 6 * tokens * units,
        ),
        compiler_params=pltpu.CompilerParams(dimension_semantics=("arbitrary",)),
        name="forward",
    )(core.reshape(1), gathered, up, down)


def hidden_kernel(core, piece, down, slopes, mine, sent, *, scale):
    summed = lax.dot_general(
        piece[...], down[...], (((0,), (0,)), ((), ())), preferred_element_type=jnp.float32
    )
    rounded = (summed * scale * slopes[...]).astype(mine.dtype)
    halves_kept(core[0], rounded, mine, sent)


def hidden_gradient(core, piece, down, slopes, scale):
    features, tokens = piece.shape
    units = down.shape[1]
    block = tokens // 2
    half = jax.ShapeDtypeStruct((tokens, units // 2), jnp.bfloat16)
    return pl.pallas_call(
        functools.partial(hidden_kernel, scale=scale),
        out_shape=(half, half),
        grid=(tokens // block,),
        in_specs=[
            pl.BlockSpec(memory_space=pltpu.SMEM),
            pl.BlockSpec((features, block), lambda i: (0, i)),
            pl.BlockSpec((features, units), lambda i: (0, 0)),
            pl.BlockSpec((block, units), lambda i: (i, 0)),
        ],
        out_specs=(
            pl.BlockSpec((block, units // 2), lambda i: (i, 0)),
            pl.BlockSpec((block, units // 2), lambda i: (i, 0)),
        ),
        cost_estimate=pl.CostEstimate(
            flops=2 * features * tokens * units,
            transcendentals=0,
            bytes_accessed=2 * features * (tokens + units) + 6 * tokens * units,
        ),
        compiler_params=pltpu.CompilerParams(dimension_semantics=("arbitrary",)),
        name="hidden_gradient",
    )(core.reshape(1), piece, down, slopes)


def from_plane(halves):
    parts = lax.all_to_all(halves, PLANE, split_axis=0, concat_axis=0, tiled=True)
    return jnp.sum(parts.astype(jnp.float32), axis=0)


def from_axis(blocks, axis):
    size = lax.axis_size(axis)
    here = lax.axis_index(axis)
    total = lax.dynamic_index_in_dim(blocks, here, 0, keepdims=False).astype(jnp.float32)
    for step in range(1, size):
        sent = lax.dynamic_index_in_dim(blocks, (here + step) % size, 0, keepdims=False)
        moved = lax.ppermute(
            sent.astype(jnp.bfloat16), axis, [(i, (i + step) % size) for i in range(size)]
        )
        total = total + moved.astype(jnp.float32)
    return total


def totals_kernel(loss, up, down, rows):
    squares = jnp.sum(up[...] * up[...]) + jnp.sum(down[...] * down[...])
    lane = lax.broadcasted_iota(jnp.int32, rows.shape, 2)
    rows[...] = jnp.where(lane < 64, loss[0], squares)


def totals(loss, up, down):
    rows = pl.pallas_call(
        totals_kernel,
        out_shape=jax.ShapeDtypeStruct((lax.axis_size(DP_MP), 1, 128), jnp.float32),
        in_specs=[
            pl.BlockSpec(memory_space=pltpu.SMEM),
            pl.BlockSpec(memory_space=pltpu.VMEM),
            pl.BlockSpec(memory_space=pltpu.VMEM),
        ],
        out_specs=pl.BlockSpec(memory_space=pltpu.VMEM),
        name="totals",
    )(loss.reshape(1), up, down)
    rows = lax.all_to_all(rows, DP_MP, split_axis=0, concat_axis=0, tiled=True)
    summed = jnp.sum(rows, axis=(0, 1))
    return summed[0], summed[64]


def over_features(left, right):
    return lax.dot_general(left, right, (((0,), (0,)), ((), ())), preferred_element_type=jnp.float32)


def gelu_pair(preact):
    tanh_arg = 0.7978845608028654 * (preact + 0.044715 * preact * preact * preact)
    tanh_val = jnp.tanh(tanh_arg)
    activation = 0.5 * preact * (1.0 + tanh_val)
    slopes = 0.5 * (1.0 + tanh_val) + 0.5 * preact * (
        1.0 - tanh_val * tanh_val
    ) * 0.7978845608028654 * (1.0 + 3.0 * 0.044715 * preact * preact)
    return (activation, slopes)


def rates(step_index, teacher_count):
    steps_float = teacher_count.astype(jnp.float32)
    doubled = 2.0 * step_index.astype(jnp.float32)
    back = jnp.arange(3, dtype=jnp.float32)[:, None]
    angles = 0.5 * math.pi * ((doubled - back) / steps_float)
    return jnp.cos(angles)[:, :, None, None], jnp.sin(angles)[:, :, None, None]


def noisy_latent(clean, noise, alphas, sigmas):
    return alphas[0] * clean.astype(jnp.float32) + sigmas[0] * noise.astype(jnp.float32)


def distill_target(latent_now, teacher_first, teacher_second, alphas, sigmas):
    alpha_now, alpha_mid, alpha_end = alphas
    sigma_now, sigma_mid, sigma_end = sigmas
    first_f = teacher_first.astype(jnp.float32)
    second_f = teacher_second.astype(jnp.float32)
    noise_now = (latent_now - alpha_now * first_f) / sigma_now
    latent_mid = alpha_mid * first_f + sigma_mid * noise_now
    noise_mid = (latent_mid - alpha_mid * second_f) / sigma_mid
    latent_end = alpha_end * second_f + sigma_end * noise_mid
    sigma_ratio = sigma_end / sigma_now
    return (latent_end - sigma_ratio * latent_now) / (alpha_end - sigma_ratio * alpha_now)


def adam_update(master, moment, second, gradient, factor):
    clipped = gradient * factor
    moment_new = 0.9 * moment + 0.1 * clipped
    second_new = 0.999 * second + 0.001 * clipped * clipped
    first_hat = moment_new / (1.0 - 0.9**adam_count)
    second_hat = second_new / (1.0 - 0.999**adam_count)
    master_new = master - learn_rate * (
        first_hat / (jnp.sqrt(second_hat) + 1e-08) + decay_rate * master
    )
    return (master_new, moment_new, second_new)


def per_device(
    clean,
    noise,
    teacher_first,
    teacher_second,
    step_index,
    teacher_count,
    up_master,
    down_master,
    up_moment,
    down_moment,
    up_second,
    down_second,
):
    samples_dev, token_count, width_local = clean.shape
    sample_total = samples_dev * lax.axis_size(DP)
    row_count = samples_dev * token_count
    alphas, sigmas = rates(step_index, teacher_count)
    weighting = jnp.maximum(alphas[0] * alphas[0] / (sigmas[0] * sigmas[0]), 1.0)
    latent = noisy_latent(clean, noise, alphas, sigmas)
    noisy_rows = latent.reshape(row_count, width_local).astype(jnp.bfloat16)
    gathered = lax.all_gather(noisy_rows.T, "mp", axis=0, tiled=True)
    *held, gathered = lax.optimization_barrier(
        (clean, noise, teacher_first, teacher_second, gathered)
    )
    latent_again = noisy_latent(*held[:2], alphas, sigmas)
    target = distill_target(latent_again, *held[2:], alphas, sigmas)
    offset = (latent_again - target).reshape(row_count, width_local).T
    up_full, down_full = gathered_weights(
        up_master.astype(jnp.bfloat16), down_master.astype(jnp.bfloat16)
    )
    width_full = up_full.shape[0]
    hidden_local = up_full.shape[1]
    dscale = width_full ** (-0.5)
    fscale = (hidden_local * lax.axis_size("mp")) ** (-0.5)
    core = lax.axis_index("c")
    normed, hidden_mine, hidden_sent, slopes, partial_value = forward(
        core, gathered, up_full, down_full, dscale, fscale
    )
    branch = lax.psum_scatter(partial_value, "mp", scatter_dimension=0, tiled=True)
    offset, normed_other, hidden_other = lax.optimization_barrier(
        (offset, core_swapped(normed), core_swapped(hidden_sent))
    )
    weight_row = jnp.repeat(weighting.reshape(samples_dev), token_count)[None]
    errors = offset + branch.astype(jnp.float32)
    loss_part = jnp.sum(weight_row * errors * errors)
    dpred = (2.0 * weight_row / sample_total * errors).astype(jnp.bfloat16)
    piece = lax.all_gather(dpred, "mp", axis=0, tiled=True)
    piece_other = core_swapped(piece)
    dpre_mine, dpre_sent = hidden_gradient(core, piece, down_full, slopes, fscale)
    dpre_other = core_swapped(dpre_sent)
    grad_down = (
        jnp.dot(piece, hidden_mine, preferred_element_type=jnp.float32)
        + jnp.dot(piece_other, hidden_other, preferred_element_type=jnp.float32)
    ) * fscale
    grad_up = (
        jnp.dot(normed, dpre_mine, preferred_element_type=jnp.float32)
        + jnp.dot(normed_other, dpre_other, preferred_element_type=jnp.float32)
    ) * dscale
    chips = lax.axis_size(PLANE)
    rows_chip = width_full // chips
    rows_down = from_plane(grad_down.astype(jnp.bfloat16).reshape(chips, rows_chip, -1))
    blocks_up = grad_up.astype(jnp.bfloat16).reshape(
        lax.axis_size("y"), lax.axis_size("x"), rows_chip, -1
    )
    rows_up = from_axis(from_axis(jnp.swapaxes(blocks_up, 0, 1), "x"), "y")
    chip_rows = jnp.stack([rows_up, rows_down])
    loss_total, square_total = totals(loss_part, rows_up, rows_down)
    by_core = chip_rows.reshape(2, 2, rows_chip // 2, -1)
    kept = lax.dynamic_index_in_dim(by_core, core, 1, keepdims=False)
    other = core_swapped(lax.dynamic_index_in_dim(by_core, 1 - core, 1, keepdims=False))
    mine_up, mine_down = jnp.where(
        core == 0, jnp.concatenate([kept, other], 2), jnp.concatenate([other, kept], 2)
    )
    clip_limit = math.sqrt(2.0 * width_full * hidden_local * lax.axis_size("mp"))
    factor = clip_limit / jnp.maximum(jnp.sqrt(square_total), clip_limit)
    new_up, up_m, up_v = adam_update(up_master, up_moment, up_second, mine_up, factor)
    new_down, down_m, down_v = adam_update(
        down_master, down_moment, down_second, mine_down, factor
    )
    loss_mean = loss_total / (sample_total * token_count * width_full)
    return (new_up, new_down, up_m, down_m, up_v, down_v, loss_mean)


def solution(mesh):
    split = Mesh(mesh.devices.reshape(4, 4, 2, mesh.shape["mp"]), DP_MP)
    placed = (
        P(DP, None, "mp"),
        P(DP, None, "mp"),
        P(DP, None, "mp"),
        P(DP, None, "mp"),
        P(DP),
        P(DP),
        P(DP, "mp"),
        P(DP, "mp"),
        P(DP, "mp"),
        P(DP, "mp"),
        P(DP, "mp"),
        P(DP, "mp"),
    )

    return jax.shard_map(
        per_device,
        mesh=split,
        in_specs=placed,
        out_specs=(
            P(DP, "mp"),
            P(DP, "mp"),
            P(DP, "mp"),
            P(DP, "mp"),
            P(DP, "mp"),
            P(DP, "mp"),
            P(),
        ),
        check_vma=False,
    )
```

```python
import functools
import math

import jax
import jax.numpy as jnp
from jax import lax
from jax.experimental import pallas as pl
from jax.experimental.pallas import tpu as pltpu
from jax.sharding import Mesh
from jax.sharding import PartitionSpec as P


DP = ("y", "x", "c")
DP_MP = ("y", "x", "c", "mp")


adam_count = 100.0
learn_rate = 0.05
decay_rate = 0.01


PLANE = ("y", "x")


def core_swapped(block):
    return lax.ppermute(block, "c", [(0, 1), (1, 0)])


def core_joined(mine, other):
    first = lax.axis_index("c") == 0
    pair = jnp.where(first, jnp.stack([mine, other], 1), jnp.stack([other, mine], 1))
    return pair.reshape(-1, mine.shape[-1])


def gathered_weights(up_rows, down_rows):
    chips = lax.axis_size(PLANE)
    rows = up_rows.shape[0]
    both = jnp.concatenate([up_rows, down_rows], axis=0)
    mine = lax.all_to_all(
        jnp.broadcast_to(both, (chips,) + both.shape), PLANE, split_axis=0, concat_axis=0, tiled=True
    )
    other = core_swapped(mine)
    return (
        core_joined(mine[:, :rows], other[:, :rows]),
        core_joined(mine[:, rows:], other[:, rows:]),
    )


def halves_kept(core, block, mine, sent):
    half = mine.shape[1]

    @pl.when(core == 0)
    def _():
        mine[...] = block[:, :half]
        sent[...] = block[:, half:]

    @pl.when(core != 0)
    def _():
        mine[...] = block[:, half:]
        sent[...] = block[:, :half]


def forward_kernel(core, gathered, up, down, normed, mine, sent, slopes, partial, *, up_scale, down_scale):
    tokens = gathered[...].astype(jnp.float32)
    mean = jnp.mean(tokens * tokens, axis=0, keepdims=True)
    rounded = (tokens * lax.rsqrt(mean + 1e-06)).astype(normed.dtype)
    normed[...] = rounded
    preact = over_features(rounded, up[...]) * up_scale
    activation, slope = gelu_pair(preact)
    slopes[...] = slope
    hidden = activation.astype(mine.dtype)
    halves_kept(core[0], hidden, mine, sent)
    summed = lax.dot_general(
        down[...], hidden, (((1,), (1,)), ((), ())), preferred_element_type=jnp.float32
    )
    partial[...] = (summed * down_scale).astype(partial.dtype)


def forward(core, gathered, up, down, up_scale, down_scale):
    features, tokens = gathered.shape
    units = up.shape[1]
    block = tokens // 4
    by_feature = pl.BlockSpec((features, block), lambda i: (0, i))
    by_half = pl.BlockSpec((block, units // 2), lambda i: (i, 0))
    whole = pl.BlockSpec((features, units), lambda i: (0, 0))
    return pl.pallas_call(
        functools.partial(forward_kernel, up_scale=up_scale, down_scale=down_scale),
        out_shape=(
            jax.ShapeDtypeStruct((features, tokens), jnp.bfloat16),
            jax.ShapeDtypeStruct((tokens, units // 2), jnp.bfloat16),
            jax.ShapeDtypeStruct((tokens, units // 2), jnp.bfloat16),
            jax.ShapeDtypeStruct((tokens, units), jnp.float32),
            jax.ShapeDtypeStruct((features, tokens), jnp.bfloat16),
        ),
        grid=(tokens // block,),
        in_specs=[pl.BlockSpec(memory_space=pltpu.SMEM), by_feature, whole, whole],
        out_specs=(
            by_feature,
            by_half,
            by_half,
            pl.BlockSpec((block, units), lambda i: (i, 0)),
            by_feature,
        ),
        cost_estimate=pl.CostEstimate(
            flops=4 * features * tokens * units,
            transcendentals=tokens * units,
            bytes_accessed=6 * features * tokens + 4 * features * units + 6 * tokens * units,
        ),
        compiler_params=pltpu.CompilerParams(dimension_semantics=("arbitrary",)),
        name="forward",
    )(core.reshape(1), gathered, up, down)


def hidden_kernel(core, piece, down, slopes, mine, sent, *, scale):
    summed = lax.dot_general(
        piece[...], down[...], (((0,), (0,)), ((), ())), preferred_element_type=jnp.float32
    )
    rounded = (summed * scale * slopes[...]).astype(mine.dtype)
    halves_kept(core[0], rounded, mine, sent)


def hidden_gradient(core, piece, down, slopes, scale):
    features, tokens = piece.shape
    units = down.shape[1]
    block = tokens // 2
    half = jax.ShapeDtypeStruct((tokens, units // 2), jnp.bfloat16)
    return pl.pallas_call(
        functools.partial(hidden_kernel, scale=scale),
        out_shape=(half, half),
        grid=(tokens // block,),
        in_specs=[
            pl.BlockSpec(memory_space=pltpu.SMEM),
            pl.BlockSpec((features, block), lambda i: (0, i)),
            pl.BlockSpec((features, units), lambda i: (0, 0)),
            pl.BlockSpec((block, units), lambda i: (i, 0)),
        ],
        out_specs=(
            pl.BlockSpec((block, units // 2), lambda i: (i, 0)),
            pl.BlockSpec((block, units // 2), lambda i: (i, 0)),
        ),
        cost_estimate=pl.CostEstimate(
            flops=2 * features * tokens * units,
            transcendentals=0,
            bytes_accessed=2 * features * (tokens + units) + 6 * tokens * units,
        ),
        compiler_params=pltpu.CompilerParams(dimension_semantics=("arbitrary",)),
        name="hidden_gradient",
    )(core.reshape(1), piece, down, slopes)


def from_axis(blocks, axis, after=None):
    size = lax.axis_size(axis)
    here = lax.axis_index(axis)
    total = lax.dynamic_index_in_dim(blocks, here, 0, keepdims=False).astype(jnp.float32)
    if after is not None:
        total, _ = lax.optimization_barrier((total, after))
    for step in range(1, size):
        sent = lax.dynamic_index_in_dim(blocks, (here + step) % size, 0, keepdims=False)
        moved = lax.ppermute(
            sent.astype(jnp.bfloat16), axis, [(i, (i + step) % size) for i in range(size)]
        )
        total = total + moved.astype(jnp.float32)
    return total


def totals_kernel(loss, up, down, rows):
    squares = jnp.sum(up[...] * up[...]) + jnp.sum(down[...] * down[...])
    lane = lax.broadcasted_iota(jnp.int32, rows.shape, 2)
    rows[...] = jnp.where(lane < 64, loss[0], squares)


def totals(loss, up, down):
    rows = pl.pallas_call(
        totals_kernel,
        out_shape=jax.ShapeDtypeStruct((lax.axis_size(DP_MP), 1, 128), jnp.float32),
        in_specs=[
            pl.BlockSpec(memory_space=pltpu.SMEM),
            pl.BlockSpec(memory_space=pltpu.VMEM),
            pl.BlockSpec(memory_space=pltpu.VMEM),
        ],
        out_specs=pl.BlockSpec(memory_space=pltpu.VMEM),
        name="totals",
    )(loss.reshape(1), up, down)
    rows = lax.all_to_all(rows, DP_MP, split_axis=0, concat_axis=0, tiled=True)
    summed = jnp.sum(rows, axis=(0, 1))
    return summed[0], summed[64]


def over_features(left, right):
    return lax.dot_general(left, right, (((0,), (0,)), ((), ())), preferred_element_type=jnp.float32)


def gelu_pair(preact):
    tanh_arg = 0.7978845608028654 * (preact + 0.044715 * preact * preact * preact)
    tanh_val = jnp.tanh(tanh_arg)
    activation = 0.5 * preact * (1.0 + tanh_val)
    slopes = 0.5 * (1.0 + tanh_val) + 0.5 * preact * (
        1.0 - tanh_val * tanh_val
    ) * 0.7978845608028654 * (1.0 + 3.0 * 0.044715 * preact * preact)
    return (activation, slopes)


def rates(step_index, teacher_count):
    steps_float = teacher_count.astype(jnp.float32)[:, None, None]
    doubled = 2.0 * step_index.astype(jnp.float32)[:, None, None]
    angles = [0.5 * math.pi * ((doubled - back) / steps_float) for back in (0.0, 1.0, 2.0)]
    return [jnp.cos(angle) for angle in angles], [jnp.sin(angle) for angle in angles]


def noisy_latent(clean, noise, alphas, sigmas):
    return alphas[0] * clean.astype(jnp.float32) + sigmas[0] * noise.astype(jnp.float32)


def distill_target(latent_now, teacher_first, teacher_second, alphas, sigmas):
    alpha_now, alpha_mid, alpha_end = alphas
    sigma_now, sigma_mid, sigma_end = sigmas
    first_f = teacher_first.astype(jnp.float32)
    second_f = teacher_second.astype(jnp.float32)
    noise_now = (latent_now - alpha_now * first_f) / sigma_now
    latent_mid = alpha_mid * first_f + sigma_mid * noise_now
    noise_mid = (latent_mid - alpha_mid * second_f) / sigma_mid
    latent_end = alpha_end * second_f + sigma_end * noise_mid
    sigma_ratio = sigma_end / sigma_now
    return (latent_end - sigma_ratio * latent_now) / (alpha_end - sigma_ratio * alpha_now)


def adam_update(master, moment, second, gradient, factor):
    clipped = gradient * factor
    moment_new = 0.9 * moment + 0.1 * clipped
    second_new = 0.999 * second + 0.001 * clipped * clipped
    first_hat = moment_new / (1.0 - 0.9**adam_count)
    second_hat = second_new / (1.0 - 0.999**adam_count)
    master_new = master - learn_rate * (
        first_hat / (jnp.sqrt(second_hat) + 1e-08) + decay_rate * master
    )
    return (master_new, moment_new, second_new)


def per_device(
    clean,
    noise,
    teacher_first,
    teacher_second,
    step_index,
    teacher_count,
    up_master,
    down_master,
    up_moment,
    down_moment,
    up_second,
    down_second,
):
    samples_dev, token_count, width_local = clean.shape
    sample_total = samples_dev * lax.axis_size(DP)
    row_count = samples_dev * token_count
    alphas, sigmas = rates(step_index, teacher_count)
    weighting = jnp.maximum(alphas[0] * alphas[0] / (sigmas[0] * sigmas[0]), 1.0)
    latent = noisy_latent(clean, noise, alphas, sigmas)
    noisy_rows = latent.reshape(row_count, width_local).astype(jnp.bfloat16)
    gathered = lax.all_gather(noisy_rows.T, "mp", axis=0, tiled=True)
    *held, gathered = lax.optimization_barrier(
        (clean, noise, teacher_first, teacher_second, gathered)
    )
    latent_again = noisy_latent(*held[:2], alphas, sigmas)
    target = distill_target(latent_again, *held[2:], alphas, sigmas)
    offset = (latent_again - target).reshape(row_count, width_local).T
    up_full, down_full = gathered_weights(
        up_master.astype(jnp.bfloat16), down_master.astype(jnp.bfloat16)
    )
    width_full = up_full.shape[0]
    hidden_local = up_full.shape[1]
    dscale = width_full ** (-0.5)
    fscale = (hidden_local * lax.axis_size("mp")) ** (-0.5)
    core = lax.axis_index("c")
    normed, hidden_mine, hidden_sent, slopes, partial_value = forward(
        core, gathered, up_full, down_full, dscale, fscale
    )
    branch = lax.psum_scatter(partial_value, "mp", scatter_dimension=0, tiled=True)
    offset, normed_other, hidden_other = lax.optimization_barrier(
        (offset, core_swapped(normed), core_swapped(hidden_sent))
    )
    weight_row = jnp.repeat(weighting.reshape(samples_dev), token_count)[None]
    errors = offset + branch.astype(jnp.float32)
    dpred = (2.0 * weight_row / sample_total * errors).astype(jnp.bfloat16)
    offset, branch, dpred = lax.optimization_barrier((offset, branch, dpred))
    errors = offset + branch.astype(jnp.float32)
    loss_part = jnp.sum(weight_row * errors * errors)
    piece, loss_part = lax.optimization_barrier(
        (lax.all_gather(dpred, "mp", axis=0, tiled=True), loss_part)
    )
    piece_other = core_swapped(piece)
    dpre_mine, dpre_sent = hidden_gradient(core, piece, down_full, slopes, fscale)
    dpre_other = core_swapped(dpre_sent)
    grad_down = (
        jnp.dot(piece, hidden_mine, preferred_element_type=jnp.float32)
        + jnp.dot(piece_other, hidden_other, preferred_element_type=jnp.float32)
    ) * fscale
    grad_up = (
        jnp.dot(normed, dpre_mine, preferred_element_type=jnp.float32)
        + jnp.dot(normed_other, dpre_other, preferred_element_type=jnp.float32)
    ) * dscale
    blocks = (lax.axis_size("y"), lax.axis_size("x"), width_full // lax.axis_size(PLANE), -1)
    sums_down = from_axis(grad_down.astype(jnp.bfloat16).reshape(blocks), "y")
    rows_down = from_axis(sums_down, "x")
    blocks_up = jnp.swapaxes(grad_up.astype(jnp.bfloat16).reshape(blocks), 0, 1)
    sums_up = from_axis(blocks_up, "x", rows_down)
    rows_up = from_axis(sums_up, "y")
    chip_rows = jnp.stack([rows_up, rows_down])
    loss_total, square_total = totals(loss_part, rows_up, rows_down)
    by_core = chip_rows.reshape(2, 2, blocks[2] // 2, -1)
    kept = lax.dynamic_index_in_dim(by_core, core, 1, keepdims=False)
    other = core_swapped(lax.dynamic_index_in_dim(by_core, 1 - core, 1, keepdims=False))
    mine_up, mine_down = jnp.where(
        core == 0, jnp.concatenate([kept, other], 2), jnp.concatenate([other, kept], 2)
    )
    clip_limit = math.sqrt(2.0 * width_full * hidden_local * lax.axis_size("mp"))
    factor = clip_limit / jnp.maximum(jnp.sqrt(square_total), clip_limit)
    new_up, up_m, up_v = adam_update(up_master, up_moment, up_second, mine_up, factor)
    new_down, down_m, down_v = adam_update(
        down_master, down_moment, down_second, mine_down, factor
    )
    loss_mean = loss_total / (sample_total * token_count * width_full)
    return (new_up, new_down, up_m, down_m, up_v, down_v, loss_mean)


def solution(mesh):
    split = Mesh(mesh.devices.reshape(4, 4, 2, mesh.shape["mp"]), DP_MP)
    placed = (
        P(DP, None, "mp"),
        P(DP, None, "mp"),
        P(DP, None, "mp"),
        P(DP, None, "mp"),
        P(DP),
        P(DP),
        P(DP, "mp"),
        P(DP, "mp"),
        P(DP, "mp"),
        P(DP, "mp"),
        P(DP, "mp"),
        P(DP, "mp"),
    )

    return jax.shard_map(
        per_device,
        mesh=split,
        in_specs=placed,
        out_specs=(
            P(DP, "mp"),
            P(DP, "mp"),
            P(DP, "mp"),
            P(DP, "mp"),
            P(DP, "mp"),
            P(DP, "mp"),
            P(),
        ),
        check_vma=False,
    )
```

```python
import functools
import math

import jax
import jax.numpy as jnp
from jax import lax
from jax.experimental import pallas as pl
from jax.experimental.pallas import tpu as pltpu
from jax.sharding import Mesh
from jax.sharding import PartitionSpec as P


DP = ("y", "x", "c")
DP_MP = ("y", "x", "c", "mp")


adam_count = 100.0
learn_rate = 0.05
decay_rate = 0.01


PLANE = ("y", "x")


def core_swapped(block):
    return lax.ppermute(block, "c", [(0, 1), (1, 0)])


def core_joined(mine, other):
    first = lax.axis_index("c") == 0
    pair = jnp.where(
        first, jnp.concatenate([mine, other], axis=1), jnp.concatenate([other, mine], axis=1)
    )
    return pair.reshape(-1, mine.shape[-1])


def gathered_weights(up_rows, down_rows):
    chips = lax.axis_size(PLANE)
    rows = up_rows.shape[0]
    both = jnp.concatenate([up_rows, down_rows], axis=0)
    mine = lax.all_to_all(
        jnp.broadcast_to(both, (chips,) + both.shape), PLANE, split_axis=0, concat_axis=0, tiled=True
    )
    other = core_swapped(mine)
    return (
        core_joined(mine[:, :rows], other[:, :rows]),
        core_joined(mine[:, rows:], other[:, rows:]),
    )


def halves_kept(core, block, mine, sent):
    half = mine.shape[1]

    @pl.when(core == 0)
    def _():
        mine[...] = block[:, :half]
        sent[...] = block[:, half:]

    @pl.when(core != 0)
    def _():
        mine[...] = block[:, half:]
        sent[...] = block[:, :half]


def forward_kernel(core, gathered, up, down, normed, mine, sent, slopes, partial, *, up_scale, down_scale):
    tokens = gathered[...].astype(jnp.float32)
    mean = jnp.mean(tokens * tokens, axis=0, keepdims=True)
    rounded = (tokens * lax.rsqrt(mean + 1e-06)).astype(normed.dtype)
    normed[...] = rounded
    preact = over_features(rounded, up[...]) * up_scale
    activation, slope = gelu_pair(preact)
    slopes[...] = slope
    hidden = activation.astype(mine.dtype)
    halves_kept(core[0], hidden, mine, sent)
    summed = lax.dot_general(
        down[...], hidden, (((1,), (1,)), ((), ())), preferred_element_type=jnp.float32
    )
    partial[...] = (summed * down_scale).astype(partial.dtype)


def forward(core, gathered, up, down, up_scale, down_scale):
    features, tokens = gathered.shape
    units = up.shape[1]
    block = tokens // 4
    by_feature = pl.BlockSpec((features, block), lambda i: (0, i))
    by_half = pl.BlockSpec((block, units // 2), lambda i: (i, 0))
    whole = pl.BlockSpec((features, units), lambda i: (0, 0))
    return pl.pallas_call(
        functools.partial(forward_kernel, up_scale=up_scale, down_scale=down_scale),
        out_shape=(
            jax.ShapeDtypeStruct((features, tokens), jnp.bfloat16),
            jax.ShapeDtypeStruct((tokens, units // 2), jnp.bfloat16),
            jax.ShapeDtypeStruct((tokens, units // 2), jnp.bfloat16),
            jax.ShapeDtypeStruct((tokens, units), jnp.float32),
            jax.ShapeDtypeStruct((features, tokens), jnp.bfloat16),
        ),
        grid=(tokens // block,),
        in_specs=[pl.BlockSpec(memory_space=pltpu.SMEM), by_feature, whole, whole],
        out_specs=(
            by_feature,
            by_half,
            by_half,
            pl.BlockSpec((block, units), lambda i: (i, 0)),
            by_feature,
        ),
        cost_estimate=pl.CostEstimate(
            flops=4 * features * tokens * units,
            transcendentals=tokens * units,
            bytes_accessed=6 * features * tokens + 4 * features * units + 6 * tokens * units,
        ),
        compiler_params=pltpu.CompilerParams(dimension_semantics=("arbitrary",)),
        name="forward",
    )(core.reshape(1), gathered, up, down)


def hidden_kernel(core, piece, down, slopes, mine, sent, *, scale):
    summed = lax.dot_general(
        piece[...], down[...], (((0,), (0,)), ((), ())), preferred_element_type=jnp.float32
    )
    rounded = (summed * scale * slopes[...]).astype(mine.dtype)
    halves_kept(core[0], rounded, mine, sent)


def hidden_gradient(core, piece, down, slopes, scale):
    features, tokens = piece.shape
    units = down.shape[1]
    block = tokens // 2
    half = jax.ShapeDtypeStruct((tokens, units // 2), jnp.bfloat16)
    return pl.pallas_call(
        functools.partial(hidden_kernel, scale=scale),
        out_shape=(half, half),
        grid=(tokens // block,),
        in_specs=[
            pl.BlockSpec(memory_space=pltpu.SMEM),
            pl.BlockSpec((features, block), lambda i: (0, i)),
            pl.BlockSpec((features, units), lambda i: (0, 0)),
            pl.BlockSpec((block, units), lambda i: (i, 0)),
        ],
        out_specs=(
            pl.BlockSpec((block, units // 2), lambda i: (i, 0)),
            pl.BlockSpec((block, units // 2), lambda i: (i, 0)),
        ),
        cost_estimate=pl.CostEstimate(
            flops=2 * features * tokens * units,
            transcendentals=0,
            bytes_accessed=2 * features * (tokens + units) + 6 * tokens * units,
        ),
        compiler_params=pltpu.CompilerParams(dimension_semantics=("arbitrary",)),
        name="hidden_gradient",
    )(core.reshape(1), piece, down, slopes)


def from_axis(blocks, axis, after=None):
    size = lax.axis_size(axis)
    here = lax.axis_index(axis)
    total = lax.dynamic_index_in_dim(blocks, here, 0, keepdims=False).astype(jnp.float32)
    if after is not None:
        total, _ = lax.optimization_barrier((total, after))
    for step in range(1, size):
        sent = lax.dynamic_index_in_dim(blocks, (here + step) % size, 0, keepdims=False)
        moved = lax.ppermute(
            sent.astype(jnp.bfloat16), axis, [(i, (i + step) % size) for i in range(size)]
        )
        total = total + moved.astype(jnp.float32)
    return total


def total(value):
    rows = jnp.broadcast_to(value, (lax.axis_size(DP_MP), 1, 128))
    rows = lax.all_to_all(rows, DP_MP, split_axis=0, concat_axis=0, tiled=True)
    return jnp.sum(rows, axis=0)


def over_features(left, right):
    return lax.dot_general(left, right, (((0,), (0,)), ((), ())), preferred_element_type=jnp.float32)


def gelu_pair(preact):
    tanh_arg = 0.7978845608028654 * (preact + 0.044715 * preact * preact * preact)
    tanh_val = jnp.tanh(tanh_arg)
    activation = 0.5 * preact * (1.0 + tanh_val)
    slopes = 0.5 * (1.0 + tanh_val) + 0.5 * preact * (
        1.0 - tanh_val * tanh_val
    ) * 0.7978845608028654 * (1.0 + 3.0 * 0.044715 * preact * preact)
    return (activation, slopes)


def rates(step_index, teacher_count):
    steps_float = teacher_count.astype(jnp.float32)[:, None, None]
    doubled = 2.0 * step_index.astype(jnp.float32)[:, None, None]
    angles = [0.5 * math.pi * ((doubled - back) / steps_float) for back in (0.0, 1.0, 2.0)]
    return [jnp.cos(angle) for angle in angles], [jnp.sin(angle) for angle in angles]


def noisy_latent(clean, noise, alphas, sigmas):
    return alphas[0] * clean.astype(jnp.float32) + sigmas[0] * noise.astype(jnp.float32)


def distill_target(latent_now, teacher_first, teacher_second, alphas, sigmas):
    alpha_now, alpha_mid, alpha_end = alphas
    sigma_now, sigma_mid, sigma_end = sigmas
    first_f = teacher_first.astype(jnp.float32)
    second_f = teacher_second.astype(jnp.float32)
    noise_now = (latent_now - alpha_now * first_f) / sigma_now
    latent_mid = alpha_mid * first_f + sigma_mid * noise_now
    noise_mid = (latent_mid - alpha_mid * second_f) / sigma_mid
    latent_end = alpha_end * second_f + sigma_end * noise_mid
    sigma_ratio = sigma_end / sigma_now
    return (latent_end - sigma_ratio * latent_now) / (alpha_end - sigma_ratio * alpha_now)


def adam_update(master, moment, second, gradient, factor):
    clipped = gradient * factor
    moment_new = 0.9 * moment + 0.1 * clipped
    second_new = 0.999 * second + 0.001 * clipped * clipped
    first_hat = moment_new / (1.0 - 0.9**adam_count)
    second_hat = second_new / (1.0 - 0.999**adam_count)
    master_new = master - learn_rate * (
        first_hat / (jnp.sqrt(second_hat) + 1e-08) + decay_rate * master
    )
    return (master_new, moment_new, second_new)


def per_device(
    clean,
    noise,
    teacher_first,
    teacher_second,
    step_index,
    teacher_count,
    up_master,
    down_master,
    up_moment,
    down_moment,
    up_second,
    down_second,
):
    samples_dev, token_count, width_local = clean.shape
    sample_total = samples_dev * lax.axis_size(DP)
    row_count = samples_dev * token_count
    alphas, sigmas = rates(step_index, teacher_count)
    weighting = jnp.maximum(alphas[0] * alphas[0] / (sigmas[0] * sigmas[0]), 1.0)
    latent = noisy_latent(clean, noise, alphas, sigmas)
    noisy_rows = latent.reshape(row_count, width_local).astype(jnp.bfloat16)
    gathered = lax.all_gather(noisy_rows.T, "mp", axis=0, tiled=True)
    *held, gathered = lax.optimization_barrier(
        (clean, noise, teacher_first, teacher_second, gathered)
    )
    latent_again = noisy_latent(*held[:2], alphas, sigmas)
    target = distill_target(latent_again, *held[2:], alphas, sigmas)
    offset = (latent_again - target).reshape(row_count, width_local).T
    up_full, down_full = gathered_weights(
        up_master.astype(jnp.bfloat16), down_master.astype(jnp.bfloat16)
    )
    width_full = up_full.shape[0]
    hidden_local = up_full.shape[1]
    dscale = width_full ** (-0.5)
    fscale = (hidden_local * lax.axis_size("mp")) ** (-0.5)
    core = lax.axis_index("c")
    normed, hidden_mine, hidden_sent, slopes, partial_value = forward(
        core, gathered, up_full, down_full, dscale, fscale
    )
    branch = lax.psum_scatter(partial_value, "mp", scatter_dimension=0, tiled=True)
    offset, normed_other, hidden_other = lax.optimization_barrier(
        (offset, core_swapped(normed), core_swapped(hidden_sent))
    )
    weight_row = jnp.repeat(weighting.reshape(samples_dev), token_count)[None]
    errors = offset + branch.astype(jnp.float32)
    dpred = (2.0 * weight_row / sample_total * errors).astype(jnp.bfloat16)
    offset, branch, dpred = lax.optimization_barrier((offset, branch, dpred))
    errors = offset + branch.astype(jnp.float32)
    loss_part = jnp.sum(weight_row * errors * errors)
    piece, loss_total = lax.optimization_barrier(
        (lax.all_gather(dpred, "mp", axis=0, tiled=True), total(loss_part))
    )
    piece_other = core_swapped(piece)
    dpre_mine, dpre_sent = hidden_gradient(core, piece, down_full, slopes, fscale)
    dpre_other = core_swapped(dpre_sent)
    grad_down = (
        jnp.dot(piece, hidden_mine, preferred_element_type=jnp.float32)
        + jnp.dot(piece_other, hidden_other, preferred_element_type=jnp.float32)
    ) * fscale
    grad_up = (
        jnp.dot(normed, dpre_mine, preferred_element_type=jnp.float32)
        + jnp.dot(normed_other, dpre_other, preferred_element_type=jnp.float32)
    ) * dscale
    blocks = (lax.axis_size("y"), lax.axis_size("x"), width_full // lax.axis_size(PLANE), -1)
    sums_down = from_axis(grad_down.astype(jnp.bfloat16).reshape(blocks), "y")
    rows_down = from_axis(sums_down, "x")
    blocks_up = jnp.swapaxes(grad_up.astype(jnp.bfloat16).reshape(blocks), 0, 1)
    sums_up = from_axis(blocks_up, "x", rows_down)
    rows_up = from_axis(sums_up, "y")
    chip_rows = jnp.stack([rows_up, rows_down])
    square_total = total(jnp.sum(rows_up * rows_up + rows_down * rows_down))
    by_core = chip_rows.reshape(2, 2, blocks[2] // 2, -1)
    kept = lax.dynamic_index_in_dim(by_core, core, 1, keepdims=False)
    other = core_swapped(lax.dynamic_index_in_dim(by_core, 1 - core, 1, keepdims=False))
    mine_up, mine_down = jnp.where(
        core == 0, jnp.concatenate([kept, other], 2), jnp.concatenate([other, kept], 2)
    )
    clip_limit = math.sqrt(2.0 * width_full * hidden_local * lax.axis_size("mp"))
    factor = clip_limit / jnp.maximum(jnp.sqrt(square_total), clip_limit)
    factor = jnp.tile(factor, (1, hidden_local // factor.shape[1]))
    new_up, up_m, up_v = adam_update(up_master, up_moment, up_second, mine_up, factor)
    new_down, down_m, down_v = adam_update(
        down_master, down_moment, down_second, mine_down, factor
    )
    loss_mean = loss_total[0, 0] / (sample_total * token_count * width_full)
    return (new_up, new_down, up_m, down_m, up_v, down_v, loss_mean)


def solution(mesh):
    split = Mesh(mesh.devices.reshape(4, 4, 2, mesh.shape["mp"]), DP_MP)
    placed = (
        P(DP, None, "mp"),
        P(DP, None, "mp"),
        P(DP, None, "mp"),
        P(DP, None, "mp"),
        P(DP),
        P(DP),
        P(DP, "mp"),
        P(DP, "mp"),
        P(DP, "mp"),
        P(DP, "mp"),
        P(DP, "mp"),
        P(DP, "mp"),
    )

    return jax.shard_map(
        per_device,
        mesh=split,
        in_specs=placed,
        out_specs=(
            P(DP, "mp"),
            P(DP, "mp"),
            P(DP, "mp"),
            P(DP, "mp"),
            P(DP, "mp"),
            P(DP, "mp"),
            P(),
        ),
        check_vma=False,
    )
```
